32 devices in a mesh: blk: 8 (over y, x, core), width: 4 (over z).
Axes of the slice: x: 2, y: 2, z: 4, core: 2. Of those that a mesh axis runs over, the one named last changes fastest.
Arguments:
- inputs: bfloat16 [8, 128, 2048], P('blk', None, 'width'), may hold values from -6 to 6
- encoder: bfloat16 [8, 2048, 4096], P('blk', 'width'), may hold values from -0.125 to 0.125
- enc_bias: float32 [8, 4096], P('blk'), may hold values from -3 to 3
- active_blocks: int32 [8, 128, 32], P('blk'), may hold values 0 or 1
- near_decoders: bfloat16 [8, 4, 4096, 2048], P('blk', None, None, 'width'), may hold values from -0.09375 to 0.09375
- far_decoders: bfloat16 [8, 2048, 2048], P('blk', None, 'width'), may hold values from -0.09375 to 0.09375
- targets: bfloat16 [8, 128, 2048], P('blk', None, 'width'), may hold values from -6 to 6
Outputs:
- reconstruction: float32 [8, 128, 2048], P('blk', None, 'width')
- grad_encoder: bfloat16 [8, 2048, 4096], P('blk', 'width')
- grad_bias: float32 [8, 4096], P('blk')
The draws below stay inside these ranges and needn't reach their ends.
All inputs are finite; a program needn't handle non-finite values. No bound on the sum of `active_blocks` on one device may be relied on, other than what follows from the above.
Results may differ from the reference program's by a relative error of at most 0.011.
Values may be sent and summed in bfloat16 or wider, within the bound.
A program may use at most 128 MiB of HBM per device.

```python
import jax
import jax.numpy as jnp

D = 2048
F = 4096
FBLK = 128
TOK = 128
LAYERS = 8
NEAR = 4
FB = 32


def plant(values, rng, smallest, largest):
    place = [jax.random.randint(jax.random.fold_in(rng, axis), (), 0, length) for axis, length in enumerate(values.shape)]
    main_axis = values.shape.index(max(values.shape))
    neighbour = place[:main_axis] + [(place[main_axis] + 1) % values.shape[main_axis]] + place[main_axis + 1:]
    return values.at[tuple(place)].set(smallest).at[tuple(neighbour)].set(largest)


def block_levels(stream_key, shape, split, least, high):
    level, own = 1.0, jax.random.fold_in(stream_key, 6)
    for dim, shards_of in split:
        heights = jnp.exp(jax.random.uniform(jax.random.fold_in(own, dim), (shards_of,), jnp.float32, least / len(split), high / len(split)))
        level = level * jnp.repeat(heights, shape[dim] // shards_of).reshape([-1 if axis == dim else 1 for axis in range(len(shape))])
    return level


def gaussian(own_key, dims, width, reach, shards=(), kind=jnp.bfloat16):
    entries = width * jax.random.normal(own_key, dims, jnp.float32)
    if shards:
        entries = entries * block_levels(own_key, dims, shards, -0.22, 0.18)
    return jnp.clip(entries, -reach, reach).astype(kind)


def setup_inputs(seed: int = 0) -> dict:
    arg_keys = jax.random.split(jax.random.key(seed), 8)
    inputs = gaussian(arg_keys[0], (LAYERS, TOK, D), 1.0, 6.0, ((0, 8), (2, 4)))
    encoder = gaussian(arg_keys[1], (LAYERS, D, F), D ** -0.5, 0.125, ((0, 8), (1, 4)))
    enc_bias = gaussian(arg_keys[2], (LAYERS, F), 0.5, 3.0, ((0, 8),), jnp.float32)
    active_blocks = plant((jax.random.randint(arg_keys[3], (LAYERS, TOK, FB), 0, 2) < 1).astype(jnp.int32), jax.random.fold_in(arg_keys[3], 1), 0, 1)
    near_decoders = gaussian(arg_keys[4], (LAYERS, NEAR, F, D), F ** -0.5, 0.09375, ((0, 8), (3, 4)))
    far_decoders = gaussian(arg_keys[5], (LAYERS, F // 2, D), F ** -0.5, 0.09375, ((0, 8), (2, 4)))
    targets = gaussian(arg_keys[6], (LAYERS, TOK, D), 1.0, 6.0, ((0, 8), (2, 4)))
    return {"inputs": inputs, "encoder": encoder, "enc_bias": enc_bias, "active_blocks": active_blocks, "near_decoders": near_decoders, "far_decoders": far_decoders, "targets": targets}


def expand_mask(blocks):
    return jnp.repeat(blocks.astype(jnp.float32), FBLK, axis=-1)


def pair_decoder(near_decoders, far_decoders, lower, upper):
    layers = LAYERS
    near_count = layers // 2
    spread = upper - lower
    if spread < near_count:
        return near_decoders[upper, spread]
    if spread == near_count:
        return jnp.concatenate([far_decoders[lower], far_decoders[upper]], axis=0)
    return near_decoders[lower, lower + layers - upper]


def reference(inputs, encoder, enc_bias, active_blocks, near_decoders, far_decoders, targets):
    layers = LAYERS
    masks_all = [expand_mask(active_blocks[level]) for level in range(layers)]
    activations = []
    for level in range(layers):
        pre_value = jnp.dot(inputs[level], encoder[level], preferred_element_type=jnp.float32) + enc_bias[level]
        activations.append((masks_all[level] * pre_value).astype(jnp.bfloat16))
    recon_rows = []
    out_grads = []
    for upper in range(layers):
        total = jnp.zeros((TOK, D), jnp.float32)
        for lower in range(upper + 1):
            weights = pair_decoder(near_decoders, far_decoders, lower, upper)
            total = total + jnp.dot(activations[lower], weights, preferred_element_type=jnp.float32)
        recon_rows.append(total)
        out_grads.append((total - targets[upper].astype(jnp.float32)).astype(jnp.bfloat16))
    enc_grads = []
    bias_grads = []
    for lower in range(layers):
        total = jnp.zeros((TOK, F), jnp.float32)
        for upper in range(lower, layers):
            weights = pair_decoder(near_decoders, far_decoders, lower, upper)
            total = total + jnp.dot(out_grads[upper], weights.T, preferred_element_type=jnp.float32)
        pre_grad = (masks_all[lower] * total).astype(jnp.bfloat16)
        enc_grads.append(jnp.dot(inputs[lower].T, pre_grad, preferred_element_type=jnp.float32).astype(jnp.bfloat16))
        bias_grads.append(jnp.sum(pre_grad.astype(jnp.float32), axis=0))
    return jnp.stack(recon_rows), jnp.stack(enc_grads), jnp.stack(bias_grads)
```

```python
import functools

import jax
import jax.numpy as jnp
from jax import lax
from jax.experimental import pallas as pl
from jax.experimental.pallas import tpu as pltpu
from jax.sharding import PartitionSpec as P

BF = jnp.bfloat16
F32 = jnp.float32


def dot(a, b):
    return jnp.dot(a, b, preferred_element_type=F32)


def dot_t(a, b):
    return lax.dot_general(a, b, (((1,), (1,)), ((), ())), preferred_element_type=F32)


def step_kernel(B, W, C, FBLK, x_ref, enc_hbm, bias_ref, blocks_ref, near_hbm, far_hbm, tgt_ref,
                recon_ref, pg_ref,
                enc, near, far, z1_out, z1_in, acts, p_out, p_in, og, terms, duo, ret, own, z3_out, z3_in, pg,
                enc_sem, near_sem, far_sem, z1_s, z1_r, z2_s, z2_r, ad_s, af_s, a_r, p_s, p_r, o_s, o_r,
                d_s, d_r, r_s, r_r, z3_s, z3_r, z4_s, z4_r):
    N = B // 2
    H = W // 2
    b = lax.axis_index("blk")
    w = lax.axis_index("width")
    even = lax.rem(b, 2) == 0
    odd = lax.rem(b, 2) == 1

    def col(j):
        return pl.ds(pl.multiple_of(j * C, C), C)

    def blk(d):
        return lax.rem(w + d, W)

    def remote(src, dst, s, r, to_b, to_w):
        return pltpu.make_async_remote_copy(src_ref=src, dst_ref=dst, send_sem=s, recv_sem=r,
                                            device_id=(to_b, to_w), device_id_type=pl.DeviceIdType.MESH)

    def loop(lo, hi, body):
        def run(i, carry):
            body(i)
            return carry
        lax.fori_loop(lo, hi, run, 0)

    def enc_copy(j):
        return pltpu.make_async_copy(enc_hbm.at[:, col(j)], enc.at[:, col(j)], enc_sem.at[j])

    def near_copy(k):
        return pltpu.make_async_copy(near_hbm.at[k], near.at[k], near_sem.at[k])

    far_copy = pltpu.make_async_copy(far_hbm, far, far_sem)

    def z1(j):
        return remote(z1_out.at[j], z1_in.at[w], z1_s.at[j], z1_r.at[w], b, j)

    def z1_arrival(j):
        return remote(z1_out.at[j], z1_in.at[j], z1_s.at[j], z1_r.at[j], b, j)

    def z2(j):
        return remote(acts.at[0, w], acts.at[0, w], z2_s.at[j], z2_r.at[w], b, j)

    def z2_arrival(j):
        return remote(acts.at[0, j], acts.at[0, j], z2_s.at[j], z2_r.at[j], b, j)

    def z3(j):
        return remote(z3_out.at[j], z3_in.at[w], z3_s.at[j], z3_r.at[w], b, j)

    def z3_arrival(j):
        return remote(z3_out.at[j], z3_in.at[j], z3_s.at[j], z3_r.at[j], b, j)

    def z4(j):
        return remote(pg.at[w], pg.at[w], z4_s.at[j], z4_r.at[w], b, j)

    def z4_arrival(j):
        return remote(pg.at[j], pg.at[j], z4_s.at[j], z4_r.at[j], b, j)

    def act_direct(k, j):
        return remote(acts.at[0, j], acts.at[k, j], ad_s.at[k, j], a_r.at[k, j], b + k, w)

    def act_pass(k_from, k, j, to):
        return remote(acts.at[k_from, j], acts.at[k, j], af_s.at[k, j], a_r.at[k, j], to, w)

    def share(k):
        return remote(p_out.at[k], p_in.at[k], p_s.at[k], p_r.at[k], b - k + B, w)

    def out_grad(k):
        return remote(og.at[0], og.at[k], o_s.at[k], o_r.at[k], b + k - B, w)

    def duo_copy(k_from, k, j, to):
        return remote(terms.at[k_from, j], duo.at[k, j], d_s.at[k_from, j], d_r.at[k, j], to, w)

    def ret_copy(k, j, to):
        return remote(terms.at[k, j], ret.at[k, j], r_s.at[k, j], r_r.at[k, j], to, w)

    loop(1, W + 1, lambda d: enc_copy(blk(d)).start())
    for k in range(N):
        near_copy(k).start()
    far_copy.start()

    barrier = pltpu.get_barrier_semaphore()
    for d in range(1, W):
        pl.semaphore_signal(barrier, inc=1, device_id=(b, lax.rem(w + d, W)), device_id_type=pl.DeviceIdType.MESH)
    for d in range(1, B):
        pl.semaphore_signal(barrier, inc=1, device_id=(lax.rem(b + d, B), w), device_id_type=pl.DeviceIdType.MESH)
    pl.semaphore_wait(barrier, W + B - 2)

    def first(d):
        j = blk(d)
        enc_copy(j).wait()
        z1_out[j] = dot(x_ref[...], enc[:, col(j)]).astype(BF)
        z1(j).start()

    loop(1, W, first)
    enc_copy(w).wait()
    own[w] = dot(x_ref[...], enc[:, col(w)]) + bias_ref[:, col(w)]
    fb = blocks_ref.shape[1]
    row_id = lax.broadcasted_iota(jnp.int32, (fb, C), 0) - w * (C // FBLK)
    lane_id = lax.broadcasted_iota(jnp.int32, (fb, C), 1) // FBLK
    spread = jnp.where(row_id == lane_id, 1.0, 0.0).astype(BF)

    def mask():
        return dot(blocks_ref[...].astype(F32).astype(BF), spread)

    def gather1(d):
        j = blk(d)
        z1_arrival(j).wait_recv()
        own[w] += z1_in[j].astype(F32)

    loop(1, W, gather1)
    acts[0, w] = (mask() * own[w]).astype(BF)
    loop(1, W, lambda d: z2(blk(d)).start())

    def act_sends(j, act):
        for k in range(2, N, 2):
            @pl.when(b + k < B)
            def _():
                act(act_direct(k, j))

        @pl.when(even)
        def _():
            act(act_pass(0, 1, j, b + 1))

        @pl.when(odd & (b + N - 1 < B))
        def _():
            act(act_direct(N - 1, j))

        @pl.when(even & (b + N < B) & (j >= H))
        def _():
            act(act_direct(N, j))

    start = lambda c: c.start()
    end = lambda c: c.wait_send()
    act_sends(w, start)

    def gather2(d):
        j = blk(d)
        z2_arrival(j).wait_recv()
        act_sends(j, start)

    loop(1, W, gather2)
    for k in range(N):
        near_copy(k).wait()
    far_copy.wait()

    def own_term(k):
        def body(j):
            recon_ref[...] += dot(acts[0, j], near[k, col(j), :])
        return body

    def far_term(j):
        recon_ref[...] += dot(acts[0, j], far[col(j), :])

    for k in range(1, N + 1):
        @pl.when(b < k)
        def _():
            recon_ref[...] = jnp.zeros(recon_ref.shape, F32)
            if k < N:
                loop(0, W, own_term(k))
            else:
                loop(0, H, far_term)
            p_out[k] = recon_ref[...].astype(BF)
            share(k).start()

    recon_ref[...] = jnp.zeros(recon_ref.shape, F32)
    loop(0, W, own_term(0))

    def inside_term(k, j):
        if k < N:
            recon_ref[...] += dot(acts[k, j], near[k, col(j), :])
        else:
            recon_ref[...] += dot(acts[k, j], far[col(j - H), :])

    def act_forwards(k, j, act):
        if k % 2 == 0 and k < N:
            @pl.when(even)
            def _():
                act(act_pass(k, k + 1, j, b + 1))

            @pl.when(odd)
            def _():
                act(act_pass(k, k - 1, j, b - 1))
        if k == N - 1:
            @pl.when(j >= H)
            def _():
                act(act_pass(k, N, j, b + 1))

    def arrival(k, j):
        return remote(acts.at[k, j], acts.at[k, j], ad_s.at[k, j], a_r.at[k, j], b, w)

    def inner(d):
        j = blk(d)
        for k in list(range(2, N, 2)) + [N - 1, N]:
            cond = b >= k
            if k >= N - 1:
                cond = cond & even
            if k == N:
                cond = cond & (j >= H)

            @pl.when(cond)
            def _():
                arrival(k, j).wait_recv()
                act_forwards(k, j, start)
                inside_term(k, j)

    loop(0, W, inner)

    def passed(d):
        j = blk(d)
        for k in list(range(1, N, 2)) + [N]:
            cond = b >= k
            if k >= N - 1:
                cond = cond & odd
            if k == N:
                cond = cond & (j >= H)

            @pl.when(cond)
            def _():
                arrival(k, j).wait_recv()
                inside_term(k, j)

    loop(0, W, passed)
    for k in range(1, N + 1):
        @pl.when(b + k >= B)
        def _():
            remote(p_out.at[k], p_in.at[k], p_s.at[k], p_r.at[k], b, w).wait_recv()
            recon_ref[...] += p_in[k].astype(F32)

    og[0] = (recon_ref[...] - tgt_ref[...].astype(F32)).astype(BF)
    for k in range(1, N + 1):
        @pl.when(b + k >= B)
        def _():
            out_grad(k).start()

    def back(d):
        j = blk(d)
        for k in list(range(1, N, 2)) + [N] + list(range(2, N, 2)):
            cond = b >= k
            if k == N:
                cond = cond & (j >= H)

            @pl.when(cond)
            def _():
                rows = near[k, col(j), :] if k < N else far[col(j - H), :]
                terms[k, j] = dot_t(og[0], rows).astype(BF)
                duo_sends(k, j, start)

    def duo_sends(k, j, act):
        if k % 2 == 1 and k <= N - 3:
            @pl.when(even)
            def _():
                act(duo_copy(k, k + 1, j, b + 1))
        if k == 1:
            @pl.when(odd)
            def _():
                act(ret_copy(1, j, b - 1))
        if k % 2 == 1 and k >= 3:
            @pl.when(odd)
            def _():
                act(duo_copy(k, k - 1, j, b - 1))
        if k == N:
            @pl.when(odd)
            def _():
                act(duo_copy(N, N - 1, j, b - 1))

            @pl.when(even)
            def _():
                act(ret_copy(N, j, b - N))

    loop(1, W + 1, back)

    def duo_add(k, j):
        remote(duo.at[k, j], duo.at[k, j], d_s.at[k, j], d_r.at[k, j], b, w).wait_recv()
        terms[k, j] = (terms[k, j].astype(F32) + duo[k, j].astype(F32)).astype(BF)

    def down(d):
        j = blk(d)
        for k in range(2, N, 2):
            @pl.when(b >= k)
            def _():
                duo_add(k, j)
                ret_copy(k, j, b - k).start()

        @pl.when(even & (b >= N - 1))
        def _():
            @pl.when(j >= H)
            def _():
                duo_add(N - 1, j)
            ret_copy(N - 1, j, b - (N - 1)).start()

    loop(1, W + 1, down)

    for k in range(1, N + 1):
        @pl.when(b < k)
        def _():
            remote(og.at[k], og.at[k], o_s.at[k], o_r.at[k], b, w).wait_recv()

    def own_back(j):
        own[j] = dot_t(og[0], near[0, col(j), :])
        for k in range(1, N):
            @pl.when(b < k)
            def _():
                own[j] += dot_t(og[k], near[k, col(j), :])

        @pl.when((b < N) & (j < H))
        def _():
            own[j] += dot_t(og[N], far[col(j), :])

    loop(0, W, own_back)

    def ret_add(k, j):
        remote(ret.at[k, j], ret.at[k, j], r_s.at[k, j], r_r.at[k, j], b, w).wait_recv()
        own[j] += ret[k, j].astype(F32)

    def collect(j):
        @pl.when(even)
        def _():
            ret_add(1, j)
        for k in range(2, N, 2):
            @pl.when(b + k < B)
            def _():
                ret_add(k, j)

        @pl.when(odd & (b + N - 1 < B))
        def _():
            ret_add(N - 1, j)

        @pl.when(even & (b + N < B) & (j >= H))
        def _():
            ret_add(N, j)

    def third(d):
        j = blk(d)
        collect(j)
        z3_out[j] = own[j].astype(BF)
        z3(j).start()

    loop(1, W, third)
    collect(w)

    def gather3(d):
        j = blk(d)
        z3_arrival(j).wait_recv()
        own[w] += z3_in[j].astype(F32)

    loop(1, W, gather3)
    pg[w] = (mask() * own[w]).astype(BF)
    loop(1, W, lambda d: z4(blk(d)).start())
    pg_ref[:, col(w)] = pg[w]

    def gather4(d):
        j = blk(d)
        z4_arrival(j).wait_recv()
        pg_ref[:, col(j)] = pg[j]

    loop(1, W, gather4)

    def drain(d):
        j = blk(d)
        z1(j).wait_send()
        z2(j).wait_send()
        z3(j).wait_send()
        z4(j).wait_send()

    loop(1, W, drain)

    def drain_blk(j):
        act_sends(j, end)
        for k in list(range(2, N, 2)) + [N - 1]:
            cond = b >= k
            if k == N - 1:
                cond = cond & even

            @pl.when(cond)
            def _():
                act_forwards(k, j, end)
        for k in range(1, N + 1):
            cond = b >= k
            if k == N:
                cond = cond & (j >= H)

            @pl.when(cond)
            def _():
                duo_sends(k, j, end)
        for k in range(2, N, 2):
            @pl.when(b >= k)
            def _():
                ret_copy(k, j, b - k).wait_send()

        @pl.when(even & (b >= N - 1))
        def _():
            ret_copy(N - 1, j, b - (N - 1)).wait_send()

    loop(0, W, drain_blk)
    for k in range(1, N + 1):
        @pl.when(b < k)
        def _():
            share(k).wait_send()

        @pl.when(b + k >= B)
        def _():
            out_grad(k).wait_send()


def weight_kernel(x_ref, pg_ref, grad_ref, bias_ref):
    grads = pg_ref[...]
    grad_ref[...] = lax.dot_general(
        x_ref[...], grads, (((0,), (0,)), ((), ())), preferred_element_type=F32
    ).astype(BF)
    bias_ref[...] = jnp.sum(grads.astype(F32), axis=0, keepdims=True)


def on_device(B, W, inputs, encoder, enc_bias, active_blocks, near_decoders, far_decoders, targets):
    N = B // 2
    x = inputs[0]
    tok, width = x.shape
    feats = encoder.shape[2]
    half = far_decoders.shape[1]
    out_cols = targets.shape[2]
    C = feats // W
    dma = pltpu.SemaphoreType.DMA
    blocks = lambda *lead: pltpu.VMEM((*lead, tok, C), BF)
    rows = lambda *lead: pltpu.VMEM((*lead, tok, out_cols), BF)
    vmem = pl.BlockSpec(memory_space=pltpu.VMEM)
    hbm = pl.BlockSpec(memory_space=pl.ANY)
    recon, pre_grad = pl.pallas_call(
        functools.partial(step_kernel, B, W, C, feats // active_blocks.shape[2]),
        out_shape=(jax.ShapeDtypeStruct((tok, out_cols), F32), jax.ShapeDtypeStruct((tok, feats), BF)),
        in_specs=[vmem, hbm, vmem, vmem, hbm, hbm, vmem],
        out_specs=(vmem, vmem),
        scratch_shapes=[
            pltpu.VMEM((width, feats), BF),
            pltpu.VMEM((N, feats, out_cols), BF),
            pltpu.VMEM((half, out_cols), BF),
            blocks(W), blocks(W), blocks(N + 1, W),
            rows(N + 1), rows(N + 1), rows(N + 1),
            blocks(N + 1, W), blocks(N, W), blocks(N + 1, W),
            pltpu.VMEM((W, tok, C), F32),
            blocks(W), blocks(W), blocks(W),
            dma((W,)), dma((N,)), dma,
            dma((W,)), dma((W,)), dma((W,)), dma((W,)),
            dma((N + 1, W)), dma((N + 1, W)), dma((N + 1, W)),
            dma((N + 1,)), dma((N + 1,)), dma((N + 1,)), dma((N + 1,)),
            dma((N + 1, W)), dma((N, W)), dma((N + 1, W)), dma((N + 1, W)),
            dma((W,)), dma((W,)), dma((W,)), dma((W,)),
        ],
        compiler_params=pltpu.CompilerParams(
            collective_id=0, has_side_effects=True, vmem_limit_bytes=67_000_000),
        name="step",
    )(x, encoder[0], enc_bias, active_blocks[0], near_decoders[0], far_decoders[0], targets[0])
    tile = min(feats, 1024)
    enc_grad, bias_grad = pl.pallas_call(
        weight_kernel,
        grid=(feats // tile,),
        out_shape=(jax.ShapeDtypeStruct((width, feats), BF), jax.ShapeDtypeStruct((1, feats), F32)),
        in_specs=[pl.BlockSpec((tok, width), lambda i: (0, 0)), pl.BlockSpec((tok, tile), lambda i: (0, i))],
        out_specs=(pl.BlockSpec((width, tile), lambda i: (0, i)), pl.BlockSpec((1, tile), lambda i: (0, i))),
        name="weights",
    )(x, pre_grad)
    return recon[None], enc_grad[None], bias_grad


def solution(mesh):
    return jax.shard_map(
        functools.partial(on_device, mesh.shape["blk"], mesh.shape["width"]),
        mesh=mesh,
        in_specs=(
            P("blk", None, "width"),
            P("blk", "width", None),
            P("blk", None),
            P("blk", None, None),
            P("blk", None, None, "width"),
            P("blk", None, "width"),
            P("blk", None, "width"),
        ),
        out_specs=(P("blk", None, "width"), P("blk", "width", None), P("blk", None)),
        check_vma=False,
    )
```

```python
import functools

import jax
import jax.numpy as jnp
from jax import lax
from jax.experimental import pallas as pl
from jax.experimental.pallas import tpu as pltpu
from jax.sharding import PartitionSpec as P

BF = jnp.bfloat16
F32 = jnp.float32


def dot(a, b):
    return jnp.dot(a, b, preferred_element_type=F32)


def dot_t(a, b):
    return lax.dot_general(a, b, (((1,), (1,)), ((), ())), preferred_element_type=F32)


def step_kernel(B, W, C, FBLK, x_ref, enc_hbm, bias_ref, blocks_ref, near_hbm, far_hbm, tgt_ref,
                recon_ref, pg_ref,
                enc, near, far, z1_out, z1_in, acts, p_out, p_in, og, terms, duo, ret, own, z3_out, z3_in, pg,
                enc_sem, near_sem, far_sem, z1_s, z1_r, z2_s, z2_r, ad_s, af_s, a_r, p_s, p_r, o_s, o_r,
                d_s, d_r, r_s, r_r, z3_s, z3_r, z4_s, z4_r):
    N = B // 2
    H = W // 2
    b = lax.axis_index("blk")
    w = lax.axis_index("width")
    even = lax.rem(b, 2) == 0
    odd = lax.rem(b, 2) == 1
    relay = N == 4
    mid = (b >= N - 2) & (b < N) & relay
    top = (b >= B - 2) & relay
    not_mid = jnp.logical_not(mid)
    not_top = jnp.logical_not(top)

    def col(j):
        return pl.ds(pl.multiple_of(j * C, C), C)

    def blk(d):
        return lax.rem(w + d, W)

    def remote(src, dst, s, r, to_b, to_w):
        return pltpu.make_async_remote_copy(src_ref=src, dst_ref=dst, send_sem=s, recv_sem=r,
                                            device_id=(to_b, to_w), device_id_type=pl.DeviceIdType.MESH)

    def loop(lo, hi, body):
        def run(i, carry):
            body(i)
            return carry
        lax.fori_loop(lo, hi, run, 0)

    def enc_copy(j):
        return pltpu.make_async_copy(enc_hbm.at[:, col(j)], enc.at[:, col(j)], enc_sem.at[j])

    def near_copy(k):
        return pltpu.make_async_copy(near_hbm.at[k], near.at[k], near_sem.at[k])

    far_copy = pltpu.make_async_copy(far_hbm, far, far_sem)

    def z1(j):
        return remote(z1_out.at[j], z1_in.at[w], z1_s.at[j], z1_r.at[w], b, j)

    def z1_arrival(j):
        return remote(z1_out.at[j], z1_in.at[j], z1_s.at[j], z1_r.at[j], b, j)

    def z2(j):
        return remote(acts.at[0, w], acts.at[0, w], z2_s.at[j], z2_r.at[w], b, j)

    def z2_arrival(j):
        return remote(acts.at[0, j], acts.at[0, j], z2_s.at[j], z2_r.at[j], b, j)

    def z3(j):
        return remote(z3_out.at[j], z3_in.at[w], z3_s.at[j], z3_r.at[w], b, j)

    def z3_arrival(j):
        return remote(z3_out.at[j], z3_in.at[j], z3_s.at[j], z3_r.at[j], b, j)

    def z4(j):
        return remote(pg.at[w], pg.at[w], z4_s.at[j], z4_r.at[w], b, j)

    def z4_arrival(j):
        return remote(pg.at[j], pg.at[j], z4_s.at[j], z4_r.at[j], b, j)

    def act_direct(k, j):
        return remote(acts.at[0, j], acts.at[k, j], ad_s.at[k, j], a_r.at[k, j], b + k, w)

    def act_pass(k_from, k, j, to):
        return remote(acts.at[k_from, j], acts.at[k, j], af_s.at[k, j], a_r.at[k, j], to, w)

    def share(k):
        return remote(p_out.at[k], p_in.at[k], p_s.at[k], p_r.at[k], b - k + B, w)

    def out_grad(k):
        return remote(og.at[0], og.at[k], o_s.at[k], o_r.at[k], b + k - B, w)

    def duo_copy(k_from, k, j, to):
        return remote(terms.at[k_from, j], duo.at[k, j], d_s.at[k_from, j], d_r.at[k, j], to, w)

    def ret_copy(k, j, to):
        return remote(terms.at[k, j], ret.at[k, j], r_s.at[k, j], r_r.at[k, j], to, w)

    loop(1, W + 1, lambda d: enc_copy(blk(d)).start())
    for k in range(N):
        near_copy(k).start()
    far_copy.start()

    barrier = pltpu.get_barrier_semaphore()
    for d in range(1, W):
        pl.semaphore_signal(barrier, inc=1, device_id=(b, lax.rem(w + d, W)), device_id_type=pl.DeviceIdType.MESH)
    for d in range(1, B):
        pl.semaphore_signal(barrier, inc=1, device_id=(lax.rem(b + d, B), w), device_id_type=pl.DeviceIdType.MESH)
    pl.semaphore_wait(barrier, W + B - 2)

    def first(d):
        j = blk(d)
        enc_copy(j).wait()
        z1_out[j] = dot(x_ref[...], enc[:, col(j)]).astype(BF)
        z1(j).start()

    loop(1, W, first)
    enc_copy(w).wait()
    own[w] = dot(x_ref[...], enc[:, col(w)]) + bias_ref[:, col(w)]
    fb = blocks_ref.shape[1]
    row_id = lax.broadcasted_iota(jnp.int32, (fb, C), 0) - w * (C // FBLK)
    lane_id = lax.broadcasted_iota(jnp.int32, (fb, C), 1) // FBLK
    spread = jnp.where(row_id == lane_id, 1.0, 0.0).astype(BF)

    def mask():
        return dot(blocks_ref[...].astype(F32).astype(BF), spread)

    def gather1(d):
        j = blk(d)
        z1_arrival(j).wait_recv()
        own[w] += z1_in[j].astype(F32)

    loop(1, W, gather1)
    acts[0, w] = (mask() * own[w]).astype(BF)
    loop(1, W, lambda d: z2(blk(d)).start())

    def act_sends(j, act):
        for k in range(2, N, 2):
            @pl.when((b + k < B) & not_mid)
            def _():
                act(act_direct(k, j))

        @pl.when(even)
        def _():
            act(act_pass(0, 1, j, b + 1))

        @pl.when(odd & (b + N - 1 < B) & not_mid)
        def _():
            act(act_direct(N - 1, j))

        @pl.when(mid | (even & (b + N < B) & (j >= H)))
        def _():
            act(act_direct(N, j))

    start = lambda c: c.start()
    end = lambda c: c.wait_send()
    act_sends(w, start)

    def gather2(d):
        j = blk(d)
        z2_arrival(j).wait_recv()
        act_sends(j, start)

    loop(1, W, gather2)
    for k in range(N):
        near_copy(k).wait()
    far_copy.wait()

    def own_term(k):
        def body(j):
            recon_ref[...] += dot(acts[0, j], near[k, col(j), :])
        return body

    def far_term(j):
        recon_ref[...] += dot(acts[0, j], far[col(j), :])

    for k in range(1, N + 1):
        @pl.when(b < k)
        def _():
            recon_ref[...] = jnp.zeros(recon_ref.shape, F32)
            if k < N:
                loop(0, W, own_term(k))
            else:
                loop(0, H, far_term)
            p_out[k] = recon_ref[...].astype(BF)
            share(k).start()

    recon_ref[...] = jnp.zeros(recon_ref.shape, F32)
    loop(0, W, own_term(0))

    def inside_term(k, j):
        if k < N:
            recon_ref[...] += dot(acts[k, j], near[k, col(j), :])
        else:
            recon_ref[...] += dot(acts[k, j], far[col(j - H), :])

    def act_forwards(k, j, act):
        if k % 2 == 0 and k < N:
            @pl.when(even)
            def _():
                act(act_pass(k, k + 1, j, b + 1))

            @pl.when(odd)
            def _():
                act(act_pass(k, k - 1, j, b - 1))
        if k == N - 1:
            @pl.when(j >= H)
            def _():
                act(act_pass(k, N, j, b + 1))

    def arrival(k, j):
        return remote(acts.at[k, j], acts.at[k, j], ad_s.at[k, j], a_r.at[k, j], b, w)

    def relay_sends(j, act):
        act(act_pass(N, 2, j, b - 2))

        @pl.when(odd)
        def _():
            act(act_pass(N, N - 1, j, b - 1))

    def inner(d):
        j = blk(d)
        if relay:
            @pl.when(top)
            def _():
                arrival(N, j).wait_recv()
                relay_sends(j, start)

                @pl.when(j >= H)
                def _():
                    inside_term(N, j)
        for k in list(range(2, N, 2)) + [N - 1, N]:
            cond = b >= k
            if k >= N - 1:
                cond = cond & even & not_top
            if k == N:
                cond = cond & (j >= H)

            @pl.when(cond)
            def _():
                arrival(k, j).wait_recv()
                act_forwards(k, j, start)
                inside_term(k, j)

    loop(0, W, inner)

    def passed(d):
        j = blk(d)
        for k in list(range(1, N, 2)) + [N]:
            cond = b >= k
            if k == N - 1:
                cond = cond & (odd | top)
            if k == N:
                cond = cond & odd & not_top
            if k == N:
                cond = cond & (j >= H)

            @pl.when(cond)
            def _():
                arrival(k, j).wait_recv()
                inside_term(k, j)

    loop(0, W, passed)
    for k in range(1, N + 1):
        @pl.when(b + k >= B)
        def _():
            remote(p_out.at[k], p_in.at[k], p_s.at[k], p_r.at[k], b, w).wait_recv()
            recon_ref[...] += p_in[k].astype(F32)

    og[0] = (recon_ref[...] - tgt_ref[...].astype(F32)).astype(BF)
    for k in range(1, N + 1):
        @pl.when(b + k >= B)
        def _():
            out_grad(k).start()

    def back(d):
        j = blk(d)
        for k in list(range(1, N, 2)) + [N] + list(range(2, N, 2)):
            cond = b >= k
            if k == N:
                cond = cond & (j >= H)

            @pl.when(cond)
            def _():
                rows = near[k, col(j), :] if k < N else far[col(j - H), :]
                terms[k, j] = dot_t(og[0], rows).astype(BF)
                duo_sends(k, j, start)

    def duo_sends(k, j, act):
        if k % 2 == 1 and k <= N - 3:
            @pl.when(even)
            def _():
                act(duo_copy(k, k + 1, j, b + 1))
        if k == 1:
            @pl.when(odd)
            def _():
                act(ret_copy(1, j, b - 1))
        if k % 2 == 1 and k >= 3:
            @pl.when(odd)
            def _():
                act(duo_copy(k, k - 1, j, b - 1))
        if k == N:
            @pl.when(odd)
            def _():
                act(duo_copy(N, N - 1, j, b - 1))

            @pl.when(even)
            def _():
                act(ret_copy(N, j, b - N))

    loop(1, W + 1, back)

    def duo_add(k, j):
        remote(duo.at[k, j], duo.at[k, j], d_s.at[k, j], d_r.at[k, j], b, w).wait_recv()
        terms[k, j] = (terms[k, j].astype(F32) + duo[k, j].astype(F32)).astype(BF)

    def down(d):
        j = blk(d)
        for k in range(2, N, 2):
            @pl.when(b >= k)
            def _():
                duo_add(k, j)
                ret_copy(k, j, b - k).start()

        @pl.when(even & (b >= N - 1))
        def _():
            @pl.when(j >= H)
            def _():
                duo_add(N - 1, j)
            ret_copy(N - 1, j, b - (N - 1)).start()

    loop(1, W + 1, down)

    for k in range(1, N + 1):
        @pl.when(b < k)
        def _():
            remote(og.at[k], og.at[k], o_s.at[k], o_r.at[k], b, w).wait_recv()

    def own_back(j):
        own[j] = dot_t(og[0], near[0, col(j), :])
        for k in range(1, N):
            @pl.when(b < k)
            def _():
                own[j] += dot_t(og[k], near[k, col(j), :])

        @pl.when((b < N) & (j < H))
        def _():
            own[j] += dot_t(og[N], far[col(j), :])

    loop(0, W, own_back)

    def ret_add(k, j):
        remote(ret.at[k, j], ret.at[k, j], r_s.at[k, j], r_r.at[k, j], b, w).wait_recv()
        own[j] += ret[k, j].astype(F32)

    def collect(j):
        @pl.when(even)
        def _():
            ret_add(1, j)
        for k in range(2, N, 2):
            @pl.when(b + k < B)
            def _():
                ret_add(k, j)

        @pl.when(odd & (b + N - 1 < B))
        def _():
            ret_add(N - 1, j)

        @pl.when(even & (b + N < B) & (j >= H))
        def _():
            ret_add(N, j)

    def third(d):
        j = blk(d)
        collect(j)
        z3_out[j] = own[j].astype(BF)
        z3(j).start()

    loop(1, W, third)
    collect(w)

    def gather3(d):
        j = blk(d)
        z3_arrival(j).wait_recv()
        own[w] += z3_in[j].astype(F32)

    loop(1, W, gather3)
    pg[w] = (mask() * own[w]).astype(BF)
    loop(1, W, lambda d: z4(blk(d)).start())
    pg_ref[:, col(w)] = pg[w]

    def gather4(d):
        j = blk(d)
        z4_arrival(j).wait_recv()
        pg_ref[:, col(j)] = pg[j]

    loop(1, W, gather4)

    def drain(d):
        j = blk(d)
        z1(j).wait_send()
        z2(j).wait_send()
        z3(j).wait_send()
        z4(j).wait_send()

    loop(1, W, drain)

    def drain_blk(j):
        act_sends(j, end)
        for k in list(range(2, N, 2)) + [N - 1]:
            cond = b >= k
            if k == N - 1:
                cond = cond & even & not_top

            @pl.when(cond)
            def _():
                act_forwards(k, j, end)
        if relay:
            @pl.when(top)
            def _():
                relay_sends(j, end)
        for k in range(1, N + 1):
            cond = b >= k
            if k == N:
                cond = cond & (j >= H)

            @pl.when(cond)
            def _():
                duo_sends(k, j, end)
        for k in range(2, N, 2):
            @pl.when(b >= k)
            def _():
                ret_copy(k, j, b - k).wait_send()

        @pl.when(even & (b >= N - 1))
        def _():
            ret_copy(N - 1, j, b - (N - 1)).wait_send()

    loop(0, W, drain_blk)
    for k in range(1, N + 1):
        @pl.when(b < k)
        def _():
            share(k).wait_send()

        @pl.when(b + k >= B)
        def _():
            out_grad(k).wait_send()


def weight_kernel(x_ref, pg_ref, grad_ref, bias_ref):
    grads = pg_ref[...]
    grad_ref[...] = lax.dot_general(
        x_ref[...], grads, (((0,), (0,)), ((), ())), preferred_element_type=F32
    ).astype(BF)
    bias_ref[...] = jnp.sum(grads.astype(F32), axis=0, keepdims=True)


def on_device(B, W, inputs, encoder, enc_bias, active_blocks, near_decoders, far_decoders, targets):
    N = B // 2
    x = inputs[0]
    tok, width = x.shape
    feats = encoder.shape[2]
    half = far_decoders.shape[1]
    out_cols = targets.shape[2]
    C = feats // W
    dma = pltpu.SemaphoreType.DMA
    blocks = lambda *lead: pltpu.VMEM((*lead, tok, C), BF)
    rows = lambda *lead: pltpu.VMEM((*lead, tok, out_cols), BF)
    vmem = pl.BlockSpec(memory_space=pltpu.VMEM)
    hbm = pl.BlockSpec(memory_space=pl.ANY)
    recon, pre_grad = pl.pallas_call(
        functools.partial(step_kernel, B, W, C, feats // active_blocks.shape[2]),
        out_shape=(jax.ShapeDtypeStruct((tok, out_cols), F32), jax.ShapeDtypeStruct((tok, feats), BF)),
        in_specs=[vmem, hbm, vmem, vmem, hbm, hbm, vmem],
        out_specs=(vmem, vmem),
        scratch_shapes=[
            pltpu.VMEM((width, feats), BF),
            pltpu.VMEM((N, feats, out_cols), BF),
            pltpu.VMEM((half, out_cols), BF),
            blocks(W), blocks(W), blocks(N + 1, W),
            rows(N + 1), rows(N + 1), rows(N + 1),
            blocks(N + 1, W), blocks(N, W), blocks(N + 1, W),
            pltpu.VMEM((W, tok, C), F32),
            blocks(W), blocks(W), blocks(W),
            dma((W,)), dma((N,)), dma,
            dma((W,)), dma((W,)), dma((W,)), dma((W,)),
            dma((N + 1, W)), dma((N + 1, W)), dma((N + 1, W)),
            dma((N + 1,)), dma((N + 1,)), dma((N + 1,)), dma((N + 1,)),
            dma((N + 1, W)), dma((N, W)), dma((N + 1, W)), dma((N + 1, W)),
            dma((W,)), dma((W,)), dma((W,)), dma((W,)),
        ],
        compiler_params=pltpu.CompilerParams(
            collective_id=0, has_side_effects=True, vmem_limit_bytes=67_000_000),
        name="step",
    )(x, encoder[0], enc_bias, active_blocks[0], near_decoders[0], far_decoders[0], targets[0])
    tile = min(feats, 1024)
    enc_grad, bias_grad = pl.pallas_call(
        weight_kernel,
        grid=(feats // tile,),
        out_shape=(jax.ShapeDtypeStruct((width, feats), BF), jax.ShapeDtypeStruct((1, feats), F32)),
        in_specs=[pl.BlockSpec((tok, width), lambda i: (0, 0)), pl.BlockSpec((tok, tile), lambda i: (0, i))],
        out_specs=(pl.BlockSpec((width, tile), lambda i: (0, i)), pl.BlockSpec((1, tile), lambda i: (0, i))),
        name="weights",
    )(x, pre_grad)
    return recon[None], enc_grad[None], bias_grad


def solution(mesh):
    return jax.shard_map(
        functools.partial(on_device, mesh.shape["blk"], mesh.shape["width"]),
        mesh=mesh,
        in_specs=(
            P("blk", None, "width"),
            P("blk", "width", None),
            P("blk", None),
            P("blk", None, None),
            P("blk", None, None, "width"),
            P("blk", None, "width"),
            P("blk", None, "width"),
        ),
        out_specs=(P("blk", None, "width"), P("blk", "width", None), P("blk", None)),
        check_vma=False,
    )
```
